32 devices in a mesh: blk: 8 (over z, x), order: 4 (over y, core).
Axes of the slice: x: 2, y: 2, z: 4, core: 2. Of those that a mesh axis runs over, the one named last changes fastest.
Arguments:
- field: float32 [16, 512, 4096], P(None, 'blk', 'order'), may hold values from -6 to 6
- ocean_mask: int32 [512, 4096], P('blk', 'order'), may hold values from 0 to 1, as said below
- plan: int32 [512], replicated, may hold values from 0 to 384, as said below
- legendre: bfloat16 [384, 1024, 1024], P('blk', 'order'), may hold values from -0.4375 to 0.4375
Outputs:
- coefficients: float32 [1024, 16, 2, 1024], P('blk', None, None, 'order')
The draws below stay inside these ranges and needn't reach their ends.
Inputs may be any that keep to these rules, and one draw needn't show every extreme that they name: `ocean_mask`: exactly 128 cycles are all land, at the ends of the cycle order; every other cycle has an ocean point. plan is 384 exactly at the cycles that are all land, and names every slot below 384 once at the other cycles; slot p belongs to index p // 48 of blk; the cycles of one index of blk name at most 8 slots of one index, and in every draw some index of blk names exactly 8 slots of some index.
All inputs are finite; a program needn't handle non-finite values.
Results may differ from the reference program's by a relative error of at most 0.0029.
Values may be sent and summed in bfloat16 or wider, within the bound.
No kernel may reach another device: no remote copies, remote signals or barrier semaphores. Data moves between devices by JAX's collectives and lax.ppermute only.
A program may use at most 128 MiB of HBM per device.

```python
import jax
import jax.numpy as jnp
from jax import lax

NLON = 4096
M = 1024
L = 1024
FIELDS = 16
CYCLES = 512
SLOT_DEV = 48
SLOTS = 384
N_BLK = 8
N_ORDER = 4


def wet_cycles(key):
    folded = jax.random.fold_in(key, 11)
    dry_count = CYCLES - SLOTS
    south = jax.random.randint(folded, (), 0, dry_count + 1)
    cycles = jnp.arange(CYCLES, dtype=jnp.int32)
    inside = (cycles >= south) & (cycles < CYCLES - dry_count + south)
    return inside.astype(jnp.int32)


def draw_plan(key, part):
    wet = wet_cycles(key)
    counted = jnp.cumsum(wet).astype(jnp.int32) - 1
    owner_slot = counted % N_BLK * SLOT_DEV + counted // N_BLK
    return jnp.where(wet == 1, owner_slot, SLOTS).astype(jnp.int32)


def draw_ocean_mask(key, part):
    wet = wet_cycles(key)
    levels = jax.random.randint(jax.random.fold_in(key, 12), (CYCLES, NLON), 0, 10)
    cycles = jnp.arange(CYCLES, dtype=jnp.int32)[:, None]
    longitudes = jnp.arange(NLON, dtype=jnp.int32)[None, :]
    forced = longitudes == cycles * 37 % NLON
    ocean = ((levels < 7) | forced) & (wet[:, None] == 1)
    return ocean.astype(jnp.int32)


def strengthened(drawn, own_key, source, target, shards_of, factor):
    owner, partner = [(jnp.arange(drawn.shape[dim]) // (drawn.shape[dim] // shards_of)).reshape([-1 if axis == dim else 1 for axis in range(drawn.ndim)]) for dim in (source, target)]
    chosen = jax.random.permutation(own_key, shards_of)[partner]
    strong = (owner == chosen) | (owner == (partner + shards_of // 2) % shards_of)
    return jnp.where(strong, factor * drawn, drawn)


def block_scale(stream_key, shape, cuts, least, high):
    gain = 1.0
    for position, blocks in cuts:
        steps = jax.random.uniform(jax.random.fold_in(jax.random.fold_in(stream_key, 6), position), (blocks,), jnp.float32, least / len(cuts), high / len(cuts))
        gain = gain * jnp.repeat(jnp.exp(steps), shape[position] // blocks).reshape((-1,) + (1,) * (len(shape) - 1 - position))
    return gain


def noise(key, shape, deviation, bound, shards=(), kind=jnp.bfloat16):
    result = deviation * jax.random.normal(key, shape, jnp.float32)
    if shards:
        result = result * block_scale(key, shape, shards, -0.22, 0.18)
    return jnp.clip(result, -bound, bound).astype(kind)


def gaussian_with(own_key, shape, scale, bound, shards, heavy, kind=jnp.bfloat16):
    drawn = scale * jax.random.normal(own_key, shape, jnp.float32)
    if shards:
        drawn = drawn * block_scale(own_key, shape, shards, -0.22, 0.18)
    return jnp.clip(strengthened(drawn, jax.random.fold_in(own_key, 3), *heavy), -bound, bound).astype(kind)


def setup_inputs(seed: int = 0) -> dict:
    key_list = jax.random.split(jax.random.key(seed), 5)
    field = noise(key_list[0], (FIELDS, CYCLES, NLON), 1.0, 6.0, ((1, 8), (2, 4)), jnp.float32)
    ocean_mask = draw_ocean_mask(jax.random.fold_in(key_list[4], 71), 0)
    plan = draw_plan(jax.random.fold_in(key_list[4], 71), 0)
    legendre = gaussian_with(key_list[3], (SLOTS, M, L), SLOTS ** -0.5, 0.4375, ((0, 8), (1, 4)), (0, 2, 8, 2.0))
    return dict(field=field, ocean_mask=ocean_mask, plan=plan, legendre=legendre)


def reference(field, ocean_mask, plan, legendre):
    masked = field * ocean_mask.astype(jnp.float32)[None]
    holder = jnp.zeros((FIELDS, SLOTS + 1, NLON), jnp.float32)
    packed = holder.at[:, plan.astype(jnp.int32), :].set(masked)[:, :SLOTS]
    transform = jnp.fft.rfft(packed, axis=2)[:, :, :M] / jnp.sqrt(jnp.float32(NLON))
    spectrum = jnp.stack([jnp.real(transform), jnp.imag(transform)], axis=2).astype(jnp.float32).astype(jnp.bfloat16)
    width = M // N_ORDER

    def one_block(block_index):
        first = (block_index * width).astype(jnp.int32)
        table = lax.dynamic_slice_in_dim(legendre, first, width, 1).astype(jnp.float32)
        values = lax.dynamic_slice_in_dim(spectrum, first, width, 3).astype(jnp.float32)
        return jnp.einsum('pml,fpcm->lfcm', table, values)
    blocks = lax.map(one_block, jnp.arange(N_ORDER, dtype=jnp.int32))
    moved = jnp.moveaxis(blocks, 0, 3)
    return moved.reshape(L, FIELDS, 2, M)
```

```python
import functools
import math

import jax
import jax.numpy as jnp
from jax import lax
from jax.experimental import pallas as pl
from jax.experimental.pallas import tpu as pltpu
from jax.sharding import PartitionSpec as P

NLON = 4096
M = 1024
GROUP = 16
CHUNKS = 8


def trig(product, period):
    angle = (product % period).astype(jnp.float32) * (2.0 * math.pi / period)
    return jnp.cos(angle), jnp.sin(angle)


def spectrum_of(rows):
    quarter = NLON // 4
    x = [rows[:, j * quarter : (j + 1) * quarter] for j in range(4)]
    even, odd = x[0] + x[2], x[1] + x[3]
    d, t = x[0] - x[2], x[1] - x[3]
    n = jnp.arange(quarter, dtype=jnp.int32)
    scale = 1.0 / math.sqrt(NLON)
    (c1, s1), (c2, s2), (c3, s3) = [[v[None] * scale for v in trig(r * n, NLON)] for r in (1, 2, 3)]
    both, diff = (even + odd) * scale, even - odd
    real = [both, d * c1 - t * s1, diff * c2, d * c3 + t * s3]
    imag = [jnp.zeros_like(both), -d * s1 - t * c1, -diff * s2, t * c3 - d * s3]
    z = jnp.stack([jnp.concatenate([a, b], axis=1) for a, b in zip(real, imag)])
    k = jnp.arange(M // 4, dtype=jnp.int32)
    c, s = trig(n[:, None] * k[None, :], quarter)
    table = jnp.concatenate([jnp.concatenate([c, -s], axis=1), jnp.concatenate([s, c], axis=1)], axis=0)
    out = lax.dot_general(
        table, z, (((0,), (2,)), ((), ())), precision=lax.Precision.HIGH, preferred_element_type=jnp.float32
    )
    return out.astype(jnp.bfloat16).reshape(2, M, rows.shape[0])


def plan_maps(plan, slot_dev, cycle_dev):
    n_blk = lax.axis_size("blk")
    own = lax.axis_index("blk")
    cap = (cycle_dev + n_blk - 1) // n_blk
    grid = plan.reshape(n_blk, cycle_dev)
    owner = grid // slot_dev
    positions = jnp.arange(cycle_dev, dtype=jnp.int32)
    earlier = positions[None, :] < positions[:, None]
    same_owner = owner[:, :, None] == owner[:, None, :]
    rank = jnp.sum(same_owner & earlier[None], axis=2, dtype=jnp.int32)
    send_pos = owner * cap + rank
    local_pos = lax.dynamic_index_in_dim(send_pos, own, 0, keepdims=False)
    buffer_ids = jnp.arange(n_blk * cap, dtype=jnp.int32)
    send = (buffer_ids[:, None] == local_pos[None, :]).astype(jnp.bfloat16)
    source_pos = (jnp.arange(n_blk, dtype=jnp.int32)[:, None] * cap + rank).reshape(-1)
    mine = (owner == own).reshape(-1)
    slot_local = (grid % slot_dev).reshape(-1)
    slot_ids = jnp.arange(slot_dev, dtype=jnp.int32)
    slot_onehot = ((slot_local[None, :] == slot_ids[:, None]) & mine[None, :]).astype(jnp.bfloat16)
    source_onehot = (source_pos[:, None] == buffer_ids[None, :]).astype(jnp.bfloat16)
    receive = jnp.dot(slot_onehot, source_onehot, preferred_element_type=jnp.float32)
    return send, receive.astype(jnp.bfloat16)


def legendre_kernel(slots, fc, n_blk, bit_ref, table_ref, spec_ref, keep_ref, send_ref):
    depth = slots * GROUP
    spec = spec_ref[0].astype(jnp.float32)
    column = lax.broadcasted_iota(jnp.int32, (GROUP, depth), 1) % GROUP
    row = lax.broadcasted_iota(jnp.int32, (GROUP, depth), 0)
    diagonal = jnp.where(column == row, 1.0, 0.0)
    left = (spec[:, None, :] * diagonal[None]).reshape(fc * GROUP, depth).astype(jnp.bfloat16)
    table = table_ref[...].reshape(depth, table_ref.shape[2])
    out = jnp.dot(left, table, preferred_element_type=jnp.float32)
    width = out.shape[1] // n_blk
    odd = bit_ref[0] == 1
    for pair in range(n_blk // 2):
        low = out[:, 2 * pair * width : (2 * pair + 1) * width]
        high = out[:, (2 * pair + 1) * width : (2 * pair + 2) * width]
        keep_ref[pair, 0] = jnp.where(odd, high, low)
        send_ref[pair, 0] = jnp.where(odd, low, high).astype(jnp.bfloat16)


def contributions(legendre, spec, bit, first, count):
    slots, _, degrees = legendre.shape
    fc = spec.shape[1]
    n_blk = lax.axis_size("blk")
    width = degrees // n_blk
    shape = (n_blk // 2, count, fc * GROUP, width)
    block = pl.BlockSpec((n_blk // 2, 1, fc * GROUP, width), lambda i: (0, i, 0, 0))
    return pl.pallas_call(
        functools.partial(legendre_kernel, slots, fc, n_blk),
        grid=(count,),
        in_specs=[
            pl.BlockSpec(memory_space=pltpu.SMEM),
            pl.BlockSpec((slots, GROUP, degrees), lambda i: (0, first + i, 0)),
            pl.BlockSpec((1, fc, slots * GROUP), lambda i: (first + i, 0, 0)),
        ],
        out_specs=[block, block],
        out_shape=[jax.ShapeDtypeStruct(shape, jnp.float32), jax.ShapeDtypeStruct(shape, jnp.bfloat16)],
        cost_estimate=pl.CostEstimate(
            flops=2 * count * fc * GROUP * slots * GROUP * degrees,
            bytes_accessed=count * GROUP * degrees * (2 * slots + 3 * fc),
            transcendentals=0,
        ),
        name="legendre_terms",
    )(bit, legendre, spec)


def body(field, ocean_mask, plan, legendre):
    fields, cycle_dev, _ = field.shape
    slot_dev, orders, degrees = legendre.shape
    n_blk = lax.axis_size("blk")
    masked = field * ocean_mask.astype(jnp.float32)[None]
    whole = lax.all_to_all(masked, "order", split_axis=1, concat_axis=2, tiled=True)
    rows = whole.reshape(-1, NLON)
    spectrum = spectrum_of(rows).reshape(2, M, fields, -1)
    spectrum = lax.all_to_all(spectrum, "order", split_axis=1, concat_axis=3, tiled=True)
    send, receive = plan_maps(plan, slot_dev, cycle_dev)
    outgoing = jnp.einsum("qr,cmfr->qfcm", send, spectrum, preferred_element_type=jnp.float32)
    arrived = lax.all_to_all(
        outgoing.astype(jnp.bfloat16), "blk", split_axis=0, concat_axis=0, tiled=True
    )
    packed = jnp.einsum("pq,qfcm->fcpm", receive, arrived, preferred_element_type=jnp.float32)
    packed = packed.astype(jnp.bfloat16).reshape(fields * 2, slot_dev, orders // GROUP, GROUP)
    packed = packed.transpose(2, 0, 1, 3).reshape(orders // GROUP, fields * 2, slot_dev * GROUP)
    groups = orders // GROUP
    step = max(groups // CHUNKS, 1)
    bit = (lax.axis_index("blk") % 2).astype(jnp.int32).reshape(1)
    swap = [(i, i ^ 1) for i in range(n_blk)]
    alike = [[i for i in range(n_blk) if i % 2 == parity] for parity in range(2)]
    pieces = []
    for first in range(0, groups, step):
        keep, send = contributions(legendre, packed, bit, first, step)
        got = lax.ppermute(send, "blk", swap)
        terms = (keep + got.astype(jnp.float32)).astype(jnp.bfloat16)
        terms = lax.all_to_all(
            terms, "blk", split_axis=0, concat_axis=0, axis_index_groups=alike, tiled=True
        )
        pieces.append(jnp.sum(terms.astype(jnp.float32), axis=0))
    total = jnp.concatenate(pieces, axis=0)
    width = degrees // n_blk
    total = total.reshape(groups, fields, 2, GROUP, width)
    return total.transpose(4, 1, 2, 0, 3).reshape(width, fields, 2, orders)


def solution(mesh):
    placed = (P(None, "blk", "order"), P("blk", "order"), P(), P("blk", "order", None))
    return jax.shard_map(
        body, mesh=mesh, in_specs=placed, out_specs=P("blk", None, None, "order"), check_vma=False
    )
```

```python
import functools
import math

import jax
import jax.numpy as jnp
from jax import lax
from jax.experimental import pallas as pl
from jax.experimental.pallas import tpu as pltpu
from jax.sharding import PartitionSpec as P

NLON = 4096
M = 1024
GROUP = 16
CHUNKS = 8


def trig(product, period):
    angle = (product % period).astype(jnp.float32) * (2.0 * math.pi / period)
    return jnp.cos(angle), jnp.sin(angle)


def spectrum_of(rows):
    quarter = NLON // 4
    x = [rows[:, j * quarter : (j + 1) * quarter] for j in range(4)]
    even, odd = x[0] + x[2], x[1] + x[3]
    d, t = x[0] - x[2], x[1] - x[3]
    n = jnp.arange(quarter, dtype=jnp.int32)
    scale = 1.0 / math.sqrt(NLON)
    (c1, s1), (c2, s2), (c3, s3) = [[v[None] * scale for v in trig(r * n, NLON)] for r in (1, 2, 3)]
    both, diff = (even + odd) * scale, even - odd
    real = [both, d * c1 - t * s1, diff * c2, d * c3 + t * s3]
    imag = [jnp.zeros_like(both), -d * s1 - t * c1, -diff * s2, t * c3 - d * s3]
    z = jnp.stack([jnp.concatenate([a, b], axis=1) for a, b in zip(real, imag)])
    k = jnp.arange(M // 4, dtype=jnp.int32)
    c, s = trig(n[:, None] * k[None, :], quarter)
    table = jnp.concatenate([jnp.concatenate([c, -s], axis=1), jnp.concatenate([s, c], axis=1)], axis=0)
    out = lax.dot_general(
        table, z, (((0,), (2,)), ((), ())), precision=lax.Precision.HIGH, preferred_element_type=jnp.float32
    )
    return out.astype(jnp.bfloat16).reshape(2, M, rows.shape[0])


def plan_maps(plan, slot_dev, cycle_dev):
    n_blk = lax.axis_size("blk")
    own = lax.axis_index("blk")
    cap = (cycle_dev + n_blk - 1) // n_blk
    grid = plan.reshape(n_blk, cycle_dev)
    owner = grid // slot_dev
    positions = jnp.arange(cycle_dev, dtype=jnp.int32)
    earlier = positions[None, :] < positions[:, None]
    same_owner = owner[:, :, None] == owner[:, None, :]
    rank = jnp.sum(same_owner & earlier[None], axis=2, dtype=jnp.int32)
    send_pos = owner * cap + rank
    local_pos = lax.dynamic_index_in_dim(send_pos, own, 0, keepdims=False)
    buffer_ids = jnp.arange(n_blk * cap, dtype=jnp.int32)
    send = (buffer_ids[:, None] == local_pos[None, :]).astype(jnp.bfloat16)
    source_pos = (jnp.arange(n_blk, dtype=jnp.int32)[:, None] * cap + rank).reshape(-1)
    mine = (owner == own).reshape(-1)
    slot_local = (grid % slot_dev).reshape(-1)
    slot_ids = jnp.arange(slot_dev, dtype=jnp.int32)
    slot_onehot = ((slot_local[None, :] == slot_ids[:, None]) & mine[None, :]).astype(jnp.bfloat16)
    source_onehot = (source_pos[:, None] == buffer_ids[None, :]).astype(jnp.bfloat16)
    receive = jnp.dot(slot_onehot, source_onehot, preferred_element_type=jnp.float32)
    return send, receive.astype(jnp.bfloat16)


def legendre_kernel(slots, fc, n_blk, bit_ref, table_ref, spec_ref, keep_ref, send_ref):
    depth = slots * GROUP
    spec = spec_ref[0].astype(jnp.float32)
    column = lax.broadcasted_iota(jnp.int32, (GROUP, depth), 1) % GROUP
    row = lax.broadcasted_iota(jnp.int32, (GROUP, depth), 0)
    diagonal = jnp.where(column == row, 1.0, 0.0)
    left = (spec[:, None, :] * diagonal[None]).reshape(fc * GROUP, depth).astype(jnp.bfloat16)
    table = table_ref[...].reshape(depth, table_ref.shape[2])
    out = jnp.dot(left, table, preferred_element_type=jnp.float32)
    width = out.shape[1] // n_blk
    odd = bit_ref[0] == 1
    for pair in range(n_blk // 2):
        low = out[:, 2 * pair * width : (2 * pair + 1) * width]
        high = out[:, (2 * pair + 1) * width : (2 * pair + 2) * width]
        keep_ref[pair, 0] = jnp.where(odd, high, low)
        send_ref[pair, 0] = jnp.where(odd, low, high).astype(jnp.bfloat16)


def contributions(legendre, spec, bit, first, count):
    slots, _, degrees = legendre.shape
    fc = spec.shape[1]
    n_blk = lax.axis_size("blk")
    width = degrees // n_blk
    shape = (n_blk // 2, count, fc * GROUP, width)
    block = pl.BlockSpec((n_blk // 2, 1, fc * GROUP, width), lambda i: (0, i, 0, 0))
    return pl.pallas_call(
        functools.partial(legendre_kernel, slots, fc, n_blk),
        grid=(count,),
        in_specs=[
            pl.BlockSpec(memory_space=pltpu.SMEM),
            pl.BlockSpec((slots, GROUP, degrees), lambda i: (0, first + i, 0)),
            pl.BlockSpec((1, fc, slots * GROUP), lambda i: (first + i, 0, 0)),
        ],
        out_specs=[block, block],
        out_shape=[jax.ShapeDtypeStruct(shape, jnp.float32), jax.ShapeDtypeStruct(shape, jnp.bfloat16)],
        cost_estimate=pl.CostEstimate(
            flops=2 * count * fc * GROUP * slots * GROUP * degrees,
            bytes_accessed=count * GROUP * degrees * (2 * slots + 3 * fc),
            transcendentals=0,
        ),
        name="legendre_terms",
    )(bit, legendre, spec)


def body(field, ocean_mask, plan, legendre):
    fields, cycle_dev, _ = field.shape
    slot_dev, orders, degrees = legendre.shape
    n_blk = lax.axis_size("blk")
    masked = field * ocean_mask.astype(jnp.float32)[None]
    whole = lax.all_to_all(masked, "order", split_axis=1, concat_axis=2, tiled=True)
    rows = whole.reshape(-1, NLON)
    spectrum = spectrum_of(rows).reshape(2, M, fields, -1)
    spectrum = lax.all_to_all(spectrum, "order", split_axis=1, concat_axis=3, tiled=True)
    send, receive = plan_maps(plan, slot_dev, cycle_dev)
    outgoing = jnp.einsum("qr,cmfr->qfcm", send, spectrum, preferred_element_type=jnp.float32)
    arrived = lax.all_to_all(
        outgoing.astype(jnp.bfloat16), "blk", split_axis=0, concat_axis=0, tiled=True
    )
    packed = jnp.einsum("pq,qfcm->fcpm", receive, arrived, preferred_element_type=jnp.float32)
    packed = packed.astype(jnp.bfloat16).reshape(fields * 2, slot_dev, orders // GROUP, GROUP)
    packed = packed.transpose(2, 0, 1, 3).reshape(orders // GROUP, fields * 2, slot_dev * GROUP)
    groups = orders // GROUP
    step = max(groups // CHUNKS, 1)
    bit = (lax.axis_index("blk") % 2).astype(jnp.int32).reshape(1)
    swap = [(i, i ^ 1) for i in range(n_blk)]
    own = lax.axis_index("blk")
    flight, pieces = [], []
    for first in range(0, groups, step):
        keep, send = contributions(legendre, packed, bit, first, step)
        flight.append((keep, lax.ppermute(send, "blk", swap)))
    chunks, stages = len(flight), n_blk.bit_length() - 1
    for tick in range(chunks + stages - 1):
        for stage in range(stages):
            chunk = tick - stage
            if not 0 <= chunk < chunks:
                continue
            terms = flight[chunk][0] + flight[chunk][1].astype(jnp.float32)
            if terms.shape[0] == 1:
                pieces.append(terms[0])
                continue
            distance = 2 ** (stage + 1)
            pairs = terms.reshape((terms.shape[0] // 2, 2) + terms.shape[1:])
            upper = (own // distance) % 2 == 1
            keep = jnp.where(upper, pairs[:, 1], pairs[:, 0])
            send = jnp.where(upper, pairs[:, 0], pairs[:, 1]).astype(jnp.bfloat16)
            far = [(i, i ^ distance) for i in range(n_blk)]
            got = lax.ppermute(send, "blk", far)
            if stage > 0 and tick + 1 < chunks:
                ahead, coming = flight[tick + 1]
                coming, keep = lax.optimization_barrier((coming, keep))
                flight[tick + 1] = (ahead, coming)
            flight[chunk] = (keep, got)
    total = jnp.concatenate(pieces, axis=0)
    width = degrees // n_blk
    total = total.reshape(groups, fields, 2, GROUP, width)
    return total.transpose(4, 1, 2, 0, 3).reshape(width, fields, 2, orders)


def solution(mesh):
    placed = (P(None, "blk", "order"), P("blk", "order"), P(), P("blk", "order", None))
    return jax.shard_map(
        body, mesh=mesh, in_specs=placed, out_specs=P("blk", None, None, "order"), check_vma=False
    )
```
